256 devices in a mesh: dp: 32 (over x, z_lo, core), tp: 8 (over z_hi, y).
Axes of the slice: x: 4, y: 4, z: 8 (z_hi: 2, z_lo: 4; z = z_hi * 4 + z_lo), core: 2. Of those that a mesh axis runs over, the one named last changes fastest.
Arguments:
- tokens: bfloat16 [8192, 2560], P('dp', 'tp'), may hold values from -16 to 16, as said below
- master: float32 [3, 14336, 2560], P(None, ('dp', 'tp')), may hold values from -1 to 1, as said below
- gradients: bfloat16 [3, 14336, 2560], P(None, ('dp', 'tp')), may hold values from -12 to 12
- first_moment: float32 [3, 14336, 2560], P(None, ('dp', 'tp')), may hold values from -6 to 6
- second_moment: float32 [3, 14336, 2560], P(None, ('dp', 'tp')), may hold values from 1 to 16
- unit_scales: float32 [2, 14336], P(None, ('dp', 'tp')), may hold values from 0.25 to 1.75
- mix_rate: float32 [2560], replicated, may hold values from 0.1 to 0.6
Outputs:
- decoded: bfloat16 [8192, 2560], P('dp', 'tp')
The draws below stay inside these ranges and needn't reach their ends.
Inputs may be any that keep to these rules, and one draw needn't show every extreme that they name: `tokens`: each token's features have root-mean-square close to one. `master`: each row of each of the three matrices has unit length.
All inputs are finite; a program needn't handle non-finite values.
Results may differ from the reference program's by a relative error of at most 0.0085.
Values may be sent and summed in bfloat16 or wider, within the bound.
No kernel may reach another device: no remote copies, remote signals or barrier semaphores. Data moves between devices by JAX's collectives and lax.ppermute only.
A program may use at most 128 MiB of HBM per device.

```python
import math
import jax
import jax.numpy as jnp
from jax import lax

D = 2560
FFW = 14336
TOKENS = 8192


def column_profile(key, spread, width_count):
    ramp_scale = jnp.exp(jnp.log(spread) * (jnp.arange(width_count, dtype=jnp.float32) / (width_count - 1) - 0.5))
    roughness = jax.random.uniform(key, (width_count,), jnp.float32, 0.6, 1.4)
    return ramp_scale * roughness


def draw_tokens(key, part):
    key_base = jax.random.fold_in(key, 11)
    key_profile = jax.random.fold_in(key, 12)
    base_values = jnp.clip(jax.random.normal(key_base, (TOKENS, D), jnp.float32), -5.0, 5.0)
    profile = column_profile(key_profile, 3.0, D)
    values = base_values * profile[None, :]
    values = values / jnp.sqrt(jnp.mean(values * values, axis=1, keepdims=True) + 1e-06)
    return values.astype(jnp.bfloat16)


def draw_master(key, part):
    key_base = jax.random.fold_in(key, 21)
    key_flat = jax.random.fold_in(key, 22)
    key_ramp = jax.random.fold_in(key, 23)
    base_values = jnp.clip(jax.random.normal(key_base, (3, FFW, D), jnp.float32), -5.0, 5.0)
    ramp = column_profile(key_ramp, 3.0, D)
    flat_scale = jax.random.uniform(key_flat, (2, 1, D), jnp.float32, 0.6, 1.4)
    profile = jnp.concatenate([flat_scale, ramp[None, None, :]], axis=0)
    values = base_values * profile
    values = values / jnp.sqrt(jnp.sum(values * values, axis=2, keepdims=True) + 1e-06)
    return values.astype(jnp.float32)


def block_scale(own_key, dims, pieces, smallest, largest):
    level = 1.0
    for dim, parts in pieces:
        heights = jax.random.uniform(jax.random.fold_in(jax.random.fold_in(own_key, 6), dim), (parts,), jnp.float32, smallest / len(pieces), largest / len(pieces))
        level = level * jnp.repeat(jnp.exp(heights), dims[dim] // parts).reshape((-1,) + (1,) * (len(dims) - 1 - dim))
    return level


def noise(stream_key, dims, deviation, most, pieces=(), kind=jnp.bfloat16):
    values = jax.random.normal(stream_key, dims, jnp.float32) * deviation
    if len(pieces) > 0:
        values = block_scale(stream_key, dims, pieces, -0.22, 0.18) * values
    return jnp.clip(values, min=-most, max=most).astype(kind)


def setup_inputs(seed: int = 0) -> dict:
    key_list = jax.random.split(jax.random.key(seed), 8)
    return {
        "tokens": draw_tokens(jax.random.fold_in(key_list[7], 71), 0),
        "master": draw_master(jax.random.fold_in(key_list[7], 71), 0),
        "gradients": noise(key_list[2], (3, FFW, D), 3.0, 12.0, ((1, 256),)),
        "first_moment": noise(key_list[3], (3, FFW, D), 1.0, 6.0, ((1, 256),), jnp.float32),
        "second_moment": jnp.clip(jnp.exp(math.log(16.0) - 2.7725887 * jax.random.uniform(key_list[4], (3, FFW, D), jnp.float32) ** block_scale(key_list[4], (3, FFW, D), ((1, 256),), -0.2, 0.2)), 1.0, 16.0),
        "unit_scales": jnp.clip(1.0 + 0.15 * jax.random.normal(key_list[5], (2, FFW), jnp.float32), 0.25, 1.75),
        "mix_rate": jnp.clip(jax.random.uniform(key_list[6], (D,), jnp.float32, 0.1, 0.6), 0.1, 0.6),
    }


beta_first = 0.9
beta_second = 0.95
learn_rate = 0.02
adam_steps = 20
epsilon = 1e-06

def adam_unit(master, gradients, first_moment, second_moment):
    gradient = gradients.astype(jnp.float32)
    moment_one = beta_first * first_moment + (1.0 - beta_first) * gradient
    moment_two = beta_second * second_moment + (1.0 - beta_second) * gradient * gradient
    stepped = master - learn_rate * (moment_one / (1.0 - beta_first ** adam_steps)) / (jnp.sqrt(moment_two / (1.0 - beta_second ** adam_steps)) + 1e-08)
    lengths = jnp.sqrt(lax.optimization_barrier(jnp.sum(stepped * stepped, axis=-1, keepdims=True)) + epsilon)
    return (stepped / lengths).astype(jnp.bfloat16)

def reference(tokens, master, gradients, first_moment, second_moment, unit_scales, mix_rate):
    unit_rows = adam_unit(master, gradients, first_moment, second_moment)
    scales_bf = lax.optimization_barrier(unit_scales.astype(jnp.bfloat16)).astype(jnp.float32)
    gate_in = jnp.dot(tokens, unit_rows[0].T, preferred_element_type=jnp.float32) * scales_bf[0][None, :]
    up_in = jnp.dot(tokens, unit_rows[1].T, preferred_element_type=jnp.float32) * scales_bf[1][None, :]
    hidden = (jax.nn.silu(gate_in) * up_in).astype(jnp.bfloat16)
    branch = jnp.dot(hidden, unit_rows[2], preferred_element_type=jnp.float32)
    branch_rms = jnp.sqrt(lax.optimization_barrier(jnp.mean(branch * branch, axis=1, keepdims=True)) + epsilon)
    inputs = tokens.astype(jnp.float32)
    mix_rates = mix_rate[None, :]
    mixed_state = inputs + mix_rates * (branch / branch_rms - inputs)
    mixed_rms = jnp.sqrt(lax.optimization_barrier(jnp.mean(mixed_state * mixed_state, axis=1, keepdims=True)) + epsilon)
    return (mixed_state / mixed_rms).astype(jnp.bfloat16)
```

```python
import jax
import jax.numpy as jnp
import numpy as np
from jax import lax
from jax.sharding import Mesh
from jax.sharding import PartitionSpec as P

AXES = ("x", "z1", "z0", "core", "zh", "y")
SIZES = (4, 2, 2, 2, 2, 4)
DP = ("x", "z1", "z0", "core")
TP = ("zh", "y")


beta_first = 0.9
beta_second = 0.95
learn_rate = 0.02
adam_steps = 20
epsilon = 1e-06


def moved(value, **shift):
    names = tuple(a for a in AXES if a in shift)
    sizes = tuple(SIZES[AXES.index(a)] for a in names)
    pairs = []
    for source in np.ndindex(*sizes):
        target = tuple((s + shift[a]) % n for s, a, n in zip(source, names, sizes))
        pairs.append(tuple(int(np.ravel_multi_index(i, sizes)) for i in (source, target)))
    return lax.ppermute(value, names, pairs)


def sent_to_all(x, axis):
    copies = jnp.broadcast_to(x, (lax.axis_size(axis), *x.shape))
    return lax.all_to_all(copies, axis, split_axis=0, concat_axis=0, tiled=True)


def unit_shard(master, gradients, first_moment, second_moment, unit_scales):
    gradient = gradients.astype(jnp.float32)
    moment_one = beta_first * first_moment + (1.0 - beta_first) * gradient
    moment_two = beta_second * second_moment + (1.0 - beta_second) * gradient * gradient
    stepped = master - learn_rate * (moment_one / (1.0 - beta_first**adam_steps)) / (
        jnp.sqrt(moment_two / (1.0 - beta_second**adam_steps)) + 1e-08
    )
    lengths = jnp.sqrt(jnp.sum(stepped * stepped, axis=-1, keepdims=True) + epsilon)
    scales = unit_scales.astype(jnp.bfloat16).astype(jnp.float32)
    scales = jnp.concatenate([scales, jnp.ones_like(scales[:1])])[:, :, None]
    return (stepped * (scales / lengths)).astype(jnp.bfloat16)


def gathered_tokens(own):
    share, tokens = own.shape
    zh = lax.axis_index("zh")
    y = lax.axis_index("y")
    here = jnp.concatenate([own, moved(own, z1=1)], axis=1)
    there = jnp.concatenate([moved(own, zh=1), moved(own, z1=1, zh=1)], axis=1)
    block = jnp.stack([jnp.where(zh == 0, here, there), jnp.where(zh == 0, there, here)])
    whole = jnp.zeros((2, 4, share, 2 * tokens), own.dtype)
    for d in range(4):
        part = moved(block, y=d) if d else block
        whole = lax.dynamic_update_slice_in_dim(whole, part[:, None], (y - d) % 4, 1)
    return whole.reshape(8 * share, 2 * tokens)


def hidden_of(pieces, features):
    rows = jnp.stack([p[:2] for p in pieces], axis=1)
    rows = rows.reshape(2, -1, rows.shape[-1])
    projected = jnp.einsum("kfd,dt->kft", rows, features, preferred_element_type=jnp.float32)
    return (jax.nn.silu(projected[0]) * projected[1]).astype(jnp.bfloat16)


def shards(tokens, master, gradients, first_moment, second_moment, unit_scales, mix_rate):
    zh = lax.axis_index("zh")
    y = lax.axis_index("y")
    own_tokens = tokens.T
    share, count = own_tokens.shape
    width = 8 * share

    shard = unit_shard(master, gradients, first_moment, second_moment, unit_scales)
    row_near = [shard, moved(shard, x=1), moved(shard, x=-1), moved(shard, x=2)]
    pair = moved(shard, z0=1)
    row_far = [pair, moved(pair, x=1), moved(pair, x=-1), moved(row_near[3], z0=1)]

    mine = gathered_tokens(own_tokens)
    other = moved(mine, core=1)

    down = jnp.concatenate([p[2] for p in row_near + row_far])

    def branch_of(features):
        hidden = jnp.concatenate([hidden_of(row_near, features), hidden_of(row_far, features)])
        return jnp.einsum("fd,ft->dt", down, hidden, preferred_element_type=jnp.float32)

    sent = branch_of(other).astype(jnp.bfloat16)
    branch = branch_of(mine) + moved(sent, core=1).astype(jnp.float32)
    branch = branch.astype(jnp.bfloat16).reshape(2, 4, share, 2 * count)

    def block_for(d):
        return lax.dynamic_index_in_dim(branch, (y + d) % 4, 1, keepdims=False)

    arrived = [moved(block_for(d), y=d) for d in (2, 1, 3)]
    total = block_for(0).astype(jnp.float32)
    for a in arrived:
        total = total + a.astype(jnp.float32)
    total = total.astype(jnp.bfloat16)

    def piece_for(z1, far):
        rows = lax.dynamic_index_in_dim(total, (zh + far) % 2, 0, keepdims=False)
        return rows[:, z1 * count : (z1 + 1) * count]

    shares = piece_for(0, 0).astype(jnp.float32)
    for z1, far in ((0, 1), (1, 1), (1, 0)):
        shares = shares + moved(piece_for(z1, far), z1=z1, zh=far).astype(jnp.float32)

    inputs = own_tokens.astype(jnp.float32)
    rates = lax.dynamic_slice_in_dim(mix_rate, (zh * 4 + y) * share, share, 0)[:, None]
    kept_part = (1.0 - rates) * inputs
    moved_part = rates * shares
    sums = jnp.stack(
        [
            jnp.sum(shares * shares, axis=0),
            jnp.sum(kept_part * kept_part, axis=0),
            jnp.sum(kept_part * moved_part, axis=0),
            jnp.sum(moved_part * moved_part, axis=0),
        ]
    )
    totals = jnp.sum(sent_to_all(sums.reshape(-1), TP), axis=0).reshape(4, count)
    branch_rms = jnp.sqrt(totals[0] / width + epsilon)
    mixed_state = inputs + rates * (shares / branch_rms - inputs)
    mean_square = (
        totals[1] + 2.0 * totals[2] / branch_rms + totals[3] / (branch_rms * branch_rms)
    ) / width
    result = mixed_state / jnp.sqrt(mean_square + epsilon)
    return result.astype(jnp.bfloat16).T


def solution(mesh):
    torus = Mesh(mesh.devices.reshape(SIZES), AXES)
    rows = P(None, AXES, None)
    placed = (P(DP, TP), rows, rows, rows, rows, P(None, AXES), P())
    return jax.shard_map(
        shards, mesh=torus, in_specs=placed, out_specs=P(DP, TP), check_vma=False
    )
```
